32 devices in a mesh: gx: 4 (over y, core), gy: 4 (over z), gz: 2 (over x).
Axes of the slice: x: 2, y: 2, z: 4, core: 2. Of those that a mesh axis runs over, the one named last changes fastest.
Arguments:
- rhs: float32 [4, 32, 32, 256], P(None, 'gx', 'gy', 'gz'), may hold values from -170 to 170
- basis: bfloat16 [4, 8, 32, 32, 256], P(None, None, 'gx', 'gy', 'gz'), may hold values from -6 to 6
- inertia: float32 [32, 32, 256], P('gx', 'gy', 'gz'), may hold values from 0.5 to 2
- helm: float32 [4], replicated, may hold values from 0.2 to 1
- stiffness: float32 [8, 8], replicated, may hold values from -0.05 to 0.6, as said below
Outputs:
- solution: float32 [4, 32, 32, 256], P(None, 'gx', 'gy', 'gz')
- new_basis: bfloat16 [4, 32, 32, 256], P(None, 'gx', 'gy', 'gz')
The draws below stay inside these ranges and needn't reach their ends.
Inputs may be any that keep to these rules, and one draw needn't show every extreme that they name: `stiffness`: symmetric; every diagonal entry exceeds the sum of the magnitudes of the other entries of its row.
All inputs are finite; a program needn't handle non-finite values.
Results may differ from the reference program's by a relative error of at most 0.001.
Values sent between devices are 32-bit elements; how exact they have to be, the bound alone decides.
A program may use at most 64 MiB of HBM per device.

```python
import math
import jax
import jax.numpy as jnp
from jax import lax

ORDER = 8
SOLVES = 4
KEEP = 8
ITERS = 2
CX = 8
CY = 8
CZ = 128
NX = 32
NY = 32
NZ = 256


def block_levels(key, count, width):
    levels = jax.random.uniform(key, (SOLVES, KEEP, count), jnp.float32, -0.5, 0.5)
    return jnp.repeat(levels, width, axis=2)


def shared_basis(key):
    raw_values = jax.random.normal(jax.random.fold_in(key, 101), (SOLVES, KEEP, NX, NY, NZ), jnp.float32)
    level_x = block_levels(jax.random.fold_in(key, 105), NX // CX, CX)
    level_y = block_levels(jax.random.fold_in(key, 106), NY // CY, CY)
    level_z = block_levels(jax.random.fold_in(key, 107), NZ // CZ, CZ)
    loudness = jnp.exp(level_x[:, :, :, None, None] + level_y[:, :, None, :, None] + level_z[:, :, None, None, :])
    return jnp.clip(raw_values * loudness, -6.0, 6.0)


def draw_basis(key, part):
    return shared_basis(key).astype(jnp.bfloat16)


def draw_rhs(key, part):
    stored = shared_basis(key).astype(jnp.bfloat16).astype(jnp.float32)
    mix_key = jax.random.fold_in(key, 202)
    noise_key = jax.random.fold_in(key, 203)
    ramp_x = jnp.arange(NX, dtype=jnp.float32) / NX
    ramp_y = jnp.arange(NY, dtype=jnp.float32) / NY
    ramp_z = jnp.arange(NZ, dtype=jnp.float32) / NZ
    scaling = 3.0 ** (ramp_x[:, None, None] + ramp_y[None, :, None] + ramp_z[None, None, :] - 1.5)
    mixing = jnp.clip(jax.random.normal(mix_key, (SOLVES, KEEP), jnp.float32), -3.0, 3.0)
    noise = jnp.clip(jax.random.normal(noise_key, (SOLVES, NX, NY, NZ), jnp.float32), -4.0, 4.0)
    return scaling[None] * noise + jnp.einsum('sk,skxyz->sxyz', mixing, stored)


def draw_stiffness(key, part):
    raw_values = jax.random.uniform(jax.random.fold_in(key, 303), (ORDER, ORDER), jnp.float32, -0.05, 0.05)
    off_part = 0.5 * (raw_values + raw_values.T) * (1.0 - jnp.eye(ORDER, dtype=jnp.float32))
    row_weight = jnp.sum(jnp.abs(off_part), axis=1)
    margin = jax.random.uniform(jax.random.fold_in(key, 304), (ORDER,), jnp.float32, 0.08, 0.25)
    return off_part + jnp.diag(row_weight + margin)


def block_scale(rng, extent, cuts, smallest, largest):
    gain = 1.0
    for axis_at, shards_of in cuts:
        draws = jax.random.uniform(jax.random.fold_in(jax.random.fold_in(rng, 6), axis_at), (shards_of,), jnp.float32, smallest / len(cuts), largest / len(cuts))
        gain = gain * jnp.repeat(jnp.exp(draws), extent[axis_at] // shards_of).reshape((-1,) + (1,) * (len(extent) - 1 - axis_at))
    return gain


def setup_inputs(seed: int = 0) -> dict:
    keys = jax.random.split(jax.random.key(seed), 6)
    return {
        "rhs": draw_rhs(jax.random.fold_in(keys[5], 71), 0),
        "basis": draw_basis(jax.random.fold_in(keys[5], 71), 0),
        "inertia": jnp.clip(jnp.exp(math.log(2.0) - 1.3862944 * jax.random.uniform(keys[2], (NX, NY, NZ), jnp.float32) ** block_scale(keys[2], (NX, NY, NZ), ((0, 4), (1, 4), (2, 2)), -0.2, 0.2)), 0.5, 2.0),
        "helm": jnp.clip(jnp.exp(jax.random.uniform(keys[3], (SOLVES,), jnp.float32, math.log(0.2), math.log(1.0))), 0.2, 1.0),
        "stiffness": draw_stiffness(jax.random.fold_in(keys[5], 71), 0),
    }


penalty = 0.15
epsilon = 1e-06
highest = lax.Precision.HIGHEST

def stiffen(vector, stiffness):
    leading, size_a, size_b, size_c = vector.shape
    points = stiffness.shape[0]
    along_a = jnp.einsum('ij,sajbc->saibc', stiffness, vector.reshape(leading, size_a // points, points, size_b, size_c), precision=highest).reshape(vector.shape)
    along_b = jnp.einsum('ij,sabjc->sabic', stiffness, vector.reshape(leading, size_a, size_b // points, points, size_c), precision=highest).reshape(vector.shape)
    along_c = jnp.einsum('ij,sabcj->sabci', stiffness, vector.reshape(leading, size_a, size_b, size_c // points, points), precision=highest).reshape(vector.shape)
    return along_a + along_b + along_c

def face_terms(vector, padded, points):
    accumulated = jnp.zeros_like(vector)
    neighbours = ((1, padded[:, 2:, 1:-1, 1:-1], padded[:, :-2, 1:-1, 1:-1]), (2, padded[:, 1:-1, 2:, 1:-1], padded[:, 1:-1, :-2, 1:-1]), (3, padded[:, 1:-1, 1:-1, 2:], padded[:, 1:-1, 1:-1, :-2]))
    for axis_pos, higher, lower_side in neighbours:
        position = lax.broadcasted_iota(jnp.int32, vector.shape, axis_pos) % points
        accumulated = accumulated + jnp.where(position == points - 1, vector - higher, 0.0)
        accumulated = accumulated + jnp.where(position == 0, vector - lower_side, 0.0)
    return accumulated

def operate(vector, padded, diagonal, stiffness):
    return diagonal * vector + stiffen(vector, stiffness) + penalty * face_terms(vector, padded, stiffness.shape[0])

def reference(rhs, basis, inertia, helm, stiffness):
    point_count = float(rhs.shape[1] * rhs.shape[2] * rhs.shape[3])
    solutions = []
    new_bases = []
    for solve_index in range(SOLVES):
        right_side = rhs[solve_index][None]
        stored = basis[solve_index].astype(jnp.float32)
        diagonal = (helm[solve_index] * inertia)[None]

        def apply_here(vector):
            padded = jnp.pad(vector, ((0, 0), (1, 1), (1, 1), (1, 1)))
            return operate(vector, padded, diagonal, stiffness)
        coefficients = jnp.einsum('kxyz,sxyz->k', stored, right_side, precision=highest) / point_count
        iterate = jnp.einsum('k,kxyz->xyz', coefficients, stored, precision=highest)[None]
        residual = right_side - apply_here(iterate)
        direction = residual
        norm_now = jnp.sum(residual * residual)
        for iteration in range(ITERS):
            image_vec = apply_here(direction)
            step_size = norm_now / jnp.sum(direction * image_vec)
            iterate = iterate + step_size * direction
            residual = residual - step_size * image_vec
            norm_next = jnp.sum(residual * residual)
            direction = residual + norm_next / norm_now * direction
            norm_now = norm_next
        weights = jnp.einsum('kxyz,sxyz->k', stored, iterate, precision=highest) / point_count
        remainder = iterate[0] - jnp.einsum('k,kxyz->xyz', weights, stored, precision=highest)
        spread = jnp.mean(remainder * remainder)
        solutions.append(iterate[0])
        new_bases.append((remainder / jnp.sqrt(spread + epsilon)).astype(jnp.bfloat16))
    return (jnp.stack(solutions), jnp.stack(new_bases))
```

```python
import functools

import jax
import jax.numpy as jnp
from jax import lax
from jax.experimental import pallas as pl
from jax.experimental.pallas import tpu as pltpu
from jax.sharding import PartitionSpec as P

penalty = 0.15
epsilon = 1e-06
highest = lax.Precision.HIGHEST
AXES = ("gx", "gy", "gz")
MESH = pl.DeviceIdType.MESH
LANES = 128
SUBLANES = 8
EXCHANGES = 3


def offsets(sizes):
    return [
        (a, b, c)
        for a in range(sizes[0])
        for b in range(sizes[1])
        for c in range(sizes[2])
        if a or b or c
    ]


def iota(shape, dim):
    return lax.broadcasted_iota(jnp.int32, shape, dim)


def line_matrix(stiffness, row, col):
    points = stiffness.shape[0]
    size = row.shape[0]
    picks = jnp.where(row[:, :1] % points == iota((size, points), 1), 1.0, 0.0)
    spread = jnp.dot(picks, stiffness, precision=highest, preferred_element_type=jnp.float32)
    spread = lax.dot_general(
        spread, picks, (((1,), (1,)), ((), ())), precision=highest,
        preferred_element_type=jnp.float32,
    )
    inside = jnp.where(row // points == col // points, spread, 0.0)
    first, last = row % points == 0, row % points == points - 1
    ends = jnp.where(first, penalty, 0.0) + jnp.where(last, penalty, 0.0)
    inside = inside + jnp.where(row == col, ends, 0.0)
    inside = inside - jnp.where((col == row + 1) & last, penalty, 0.0)
    return inside - jnp.where((col == row - 1) & first, penalty, 0.0)


def kernel(
    sizes, total_points,
    rhs, basis, inertia, helm, stiffness,
    sol, new,
    wide, x0, r0, q, mat_z, mat_xy,
    face_y, face_z, ghost_x, ghost_y, ghost_z,
    row1, rows2, got1, got2,
    halo_send, halo_recv, send1, recv1, send2, recv2,
):
    solves, keep, size_x, size_y, size_z = basis.shape
    here = tuple(lax.axis_index(axis) for axis in AXES)
    moves = offsets(sizes)
    unrolled = len(moves) <= 64
    inverse = 1.0 / total_points

    def partner(move):
        return {
            axis: lax.rem(here[d] + move[d], sizes[d]) for d, axis in enumerate(AXES)
        }

    def for_all(act):
        if unrolled:
            for slot, move in enumerate(moves):
                act(slot, partner(move))
        else:
            def step(index, carry):
                away = index + 1
                move = (
                    away // (sizes[1] * sizes[2]),
                    (away // sizes[2]) % sizes[1],
                    away % sizes[2],
                )
                act(index, partner(move))
                return carry
            lax.fori_loop(0, len(moves), step, 0)

    ghost_x[...] = jnp.zeros_like(ghost_x)
    ghost_y[...] = jnp.zeros_like(ghost_y)
    ghost_z[...] = jnp.zeros_like(ghost_z)
    barrier = pltpu.get_barrier_semaphore()
    for_all(
        lambda slot, target: pl.semaphore_signal(
            barrier, inc=1, device_id=target, device_id_type=MESH
        )
    )

    def row_of(parts):
        stack = jnp.concatenate([jnp.sum(part, axis=0, keepdims=True) for part in parts], axis=0)
        if len(parts) < LANES:
            stack = jnp.concatenate(
                [stack, jnp.zeros((LANES - len(parts), stack.shape[1]), jnp.float32)], axis=0
            )
        return lax.dot_general(
            jnp.ones((SUBLANES, stack.shape[1]), jnp.float32), stack,
            (((1,), (1,)), ((), ())), precision=highest, preferred_element_type=jnp.float32,
        )[:1]

    def inner(a, b):
        return jnp.sum(a * b, axis=0)

    def splat(row, lane):
        return jnp.broadcast_to(row[:, lane:lane + 1], (size_y, size_z))

    def send_all(source, got, send, recv):
        def act(slot, target):
            pltpu.make_async_remote_copy(
                src_ref=source, dst_ref=got.at[slot], send_sem=send, recv_sem=recv,
                device_id=target, device_id_type=MESH,
            ).start()
        for_all(act)

    def take_all(got, send, recv):
        pltpu.make_async_copy(got, got, send).wait()
        pltpu.make_async_copy(got, got, recv).wait()

    parts = []
    for s in range(solves):
        for k in range(keep):
            stored = basis[s, k].astype(jnp.float32)
            wide[s, k] = stored
            parts.append(inner(stored, rhs[s]))
    row1[...] = row_of(parts)
    pl.semaphore_wait(barrier, len(moves))
    send_all(row1, got1, send1, recv1)

    row, col = iota((size_z, size_z), 0), iota((size_z, size_z), 1)
    mat_z[...] = line_matrix(stiffness[...], row, col)
    area = size_x * size_y
    row, col = iota((area, area), 0), iota((area, area), 1)
    row_x, col_x, row_y, col_y = row // size_y, col // size_y, row % size_y, col % size_y
    mat_xy[...] = jnp.where(
        row_y == col_y, line_matrix(stiffness[...], row_x, col_x), 0.0
    ) + jnp.where(row_x == col_x, line_matrix(stiffness[...], row_y, col_y), 0.0)
    pairs = [(k, l) for k in range(keep) for l in range(k, keep)]
    gram = [inner(wide[s, k], wide[s, l]) for s in range(solves) for k, l in pairs]
    rows2[1:2] = row_of(gram[:LANES])
    gram_rest = gram[LANES:]

    lane = iota((size_y, size_z), 1)
    sub = iota((size_y, size_z), 0)

    def exchange(index, field):
        for s in range(solves):
            for side, pos in ((0, 0), (1, size_y - 1)):
                face_y[index, side, s] = jnp.concatenate(
                    [field[s, x, pos:pos + 1, :] for x in range(size_x)], axis=0
                )
        for side, pos in ((0, 0), (1, size_z - 1)):
            pack = jnp.zeros((size_y, size_z), jnp.float32)
            for s in range(solves):
                for x in range(size_x):
                    column = jnp.broadcast_to(field[s, x, :, pos:pos + 1], (size_y, size_z))
                    pack = jnp.where(lane == s * size_x + x, column, pack)
            face_z[index, side] = pack

        def each(act):
            for d, axis in enumerate(AXES):
                if sizes[d] == 1:
                    continue
                for side, step in ((0, -1), (1, 1)):
                    if d == 0:
                        source = field.at[:, 0 if side == 0 else size_x - 1]
                        target = ghost_x.at[index, 1 - side]
                    elif d == 1:
                        source, target = face_y.at[index, side], ghost_y.at[index, 1 - side]
                    else:
                        source, target = face_z.at[index, side], ghost_z.at[index, 1 - side]
                    sends = here[d] > 0 if side == 0 else here[d] < sizes[d] - 1
                    takes = here[d] < sizes[d] - 1 if side == 0 else here[d] > 0
                    copy = pltpu.make_async_remote_copy(
                        src_ref=source, dst_ref=target,
                        send_sem=halo_send.at[index, 2 * d + side],
                        recv_sem=halo_recv.at[index, 2 * d + side],
                        device_id={axis: jnp.clip(here[d] + step, 0, sizes[d] - 1)},
                        device_id_type=MESH,
                    )
                    act(copy, sends, takes)

        def start(copy, sends, takes):
            @pl.when(sends)
            def _():
                copy.start()

        def finish(copy, sends, takes):
            @pl.when(takes)
            def _():
                copy.wait_recv()

            @pl.when(sends)
            def _():
                copy.wait_send()

        each(start)
        return lambda: each(finish)

    def local(field, s):
        flat = field[s].reshape(area, size_z)
        along_z = jnp.dot(flat, mat_z[...], precision=highest, preferred_element_type=jnp.float32)
        along_xy = jnp.dot(mat_xy[...], flat, precision=highest, preferred_element_type=jnp.float32)
        out = (along_z + along_xy).reshape(size_x, size_y, size_z)
        return out + helm[s] * inertia[...] * field[s]

    def coupled(index, s):
        low_z, high_z = ghost_z[index, 0], ghost_z[index, 1]
        planes = []
        for x in range(size_x):
            spot = s * size_x + x
            plane = jnp.where(lane == 0, jnp.broadcast_to(low_z[:, spot:spot + 1], lane.shape), 0.0)
            plane = jnp.where(
                lane == size_z - 1, jnp.broadcast_to(high_z[:, spot:spot + 1], lane.shape), plane
            )
            plane = plane + jnp.where(
                sub == 0, jnp.broadcast_to(ghost_y[index, 0, s, x:x + 1, :], lane.shape), 0.0
            )
            plane = plane + jnp.where(
                sub == size_y - 1,
                jnp.broadcast_to(ghost_y[index, 1, s, x:x + 1, :], lane.shape), 0.0,
            )
            if x == 0:
                plane = plane + ghost_x[index, 0, s]
            if x == size_x - 1:
                plane = plane + ghost_x[index, 1, s]
            planes.append(plane)
        return penalty * jnp.stack(planes)

    take_all(got1, send1, recv1)
    coefs = (row1[...] + jnp.sum(got1[...], axis=0)) * inverse
    for s in range(solves):
        total = jnp.zeros((size_x, size_y, size_z), jnp.float32)
        for k in range(keep):
            total = total + splat(coefs, s * keep + k)[None] * wide[s, k]
        x0[s] = total
    finish = exchange(0, x0)
    for s in range(solves):
        r0[s] = rhs[s] - local(x0, s)
    finish()
    for s in range(solves):
        r0[s] = r0[s] + coupled(0, s)
    finish = exchange(1, r0)
    for s in range(solves):
        q[s] = local(r0, s)
    with_r = [inner(wide[s, k], r0[s]) for s in range(solves) for k in range(keep)]
    finish()
    for s in range(solves):
        q[s] = q[s] - coupled(1, s)
    finish = exchange(2, q)
    with_q = [inner(wide[s, k], q[s]) for s in range(solves) for k in range(keep)]
    moments = []
    for s in range(solves):
        moments.append(
            [inner(r0[s], r0[s]), inner(r0[s], q[s]), inner(q[s], q[s]), inner(q[s], local(q, s))]
        )
    finish()
    for s in range(solves):
        moments[s][3] = moments[s][3] - inner(q[s], coupled(2, s))
    flat_moments = [moments[s][j] for s in range(solves) for j in range(4)]
    rows2[0:1] = row_of(with_r + with_q + flat_moments + gram_rest)
    send_all(rows2, got2, send2, recv2)
    take_all(got2, send2, recv2)
    sums = (rows2[...] + jnp.sum(got2[...], axis=0)) * inverse
    main, other = sums[0:1], sums[1:2]
    at_q, at_m = solves * keep, 2 * solves * keep
    at_rest = at_m + 4 * solves

    for s in range(solves):
        coef = [splat(coefs, s * keep + k) for k in range(keep)]
        by_r = [splat(main, s * keep + k) for k in range(keep)]
        by_q = [splat(main, at_q + s * keep + k) for k in range(keep)]
        m0, m1, m2, m3 = (splat(main, at_m + 4 * s + j) for j in range(4))
        table = {}
        for at, (k, l) in enumerate(pairs):
            spot = s * len(pairs) + at
            value = splat(other, spot) if spot < LANES else splat(main, at_rest + spot - LANES)
            table[k, l] = table[l, k] = value
        first = m0 / m1
        middle = m2 / m1
        across = m3 / m1 - middle * middle
        flat = across <= 1e-6 * middle * middle
        second = jnp.where(flat, 0.0, (1.0 - first * middle) / jnp.where(flat, 1.0, across))
        on_q = second
        on_r = first - second * middle
        moved = [
            functools.reduce(lambda a, b: a + b, [table[k, l] * coef[l] for l in range(keep)])
            for k in range(keep)
        ]
        weight = [moved[k] + on_r * by_r[k] + on_q * by_q[k] for k in range(keep)]
        square = on_r * on_r * m0 + 2.0 * on_r * on_q * m1 + on_q * on_q * m2
        mixed = jnp.zeros_like(square)
        for k in range(keep):
            square = square + coef[k] * (2.0 * weight[k] - moved[k])
            pulled = functools.reduce(
                lambda a, b: a + b, [table[k, l] * weight[l] for l in range(keep)]
            )
            mixed = mixed + weight[k] * (pulled - 2.0 * weight[k])
        scale = lax.rsqrt(square + mixed + epsilon)
        answer = x0[s] + on_r[None] * r0[s] + on_q[None] * q[s]
        sol[s] = answer
        for k in range(keep):
            answer = answer - weight[k][None] * wide[s, k]
        new[s] = (answer * scale[None]).astype(jnp.bfloat16)


def on_device(sizes, rhs, basis, inertia, helm, stiffness):
    solves, size_x, size_y, size_z = rhs.shape
    total_points = float(rhs[0].size * sizes[0] * sizes[1] * sizes[2])
    others = sizes[0] * sizes[1] * sizes[2] - 1
    field = pltpu.VMEM(rhs.shape, jnp.float32)
    vmem = pl.BlockSpec(memory_space=pltpu.VMEM)
    smem = pl.BlockSpec(memory_space=pltpu.SMEM)
    area = size_x * size_y
    faces = (EXCHANGES, 2, solves)
    return pl.pallas_call(
        functools.partial(kernel, sizes, total_points),
        out_shape=(
            jax.ShapeDtypeStruct(rhs.shape, jnp.float32),
            jax.ShapeDtypeStruct(rhs.shape, jnp.bfloat16),
        ),
        in_specs=[vmem, vmem, vmem, smem, vmem],
        out_specs=(vmem, vmem),
        scratch_shapes=[
            pltpu.VMEM(basis.shape, jnp.float32),
            field, field, field,
            pltpu.VMEM((size_z, size_z), jnp.float32),
            pltpu.VMEM((area, area), jnp.float32),
            pltpu.VMEM((*faces, size_x, size_z), jnp.float32),
            pltpu.VMEM((EXCHANGES, 2, size_y, size_z), jnp.float32),
            pltpu.VMEM((*faces, size_y, size_z), jnp.float32),
            pltpu.VMEM((*faces, size_x, size_z), jnp.float32),
            pltpu.VMEM((EXCHANGES, 2, size_y, size_z), jnp.float32),
            pltpu.VMEM((1, LANES), jnp.float32),
            pltpu.VMEM((2, LANES), jnp.float32),
            pltpu.VMEM((others, 1, LANES), jnp.float32),
            pltpu.VMEM((others, 2, LANES), jnp.float32),
            pltpu.SemaphoreType.DMA((EXCHANGES, 6)),
            pltpu.SemaphoreType.DMA((EXCHANGES, 6)),
            pltpu.SemaphoreType.DMA,
            pltpu.SemaphoreType.DMA,
            pltpu.SemaphoreType.DMA,
            pltpu.SemaphoreType.DMA,
        ],
        compiler_params=pltpu.CompilerParams(collective_id=0, has_side_effects=True),
    )(rhs, basis, inertia, helm, stiffness)


def solution(mesh):
    placed = (
        P(None, "gx", "gy", "gz"),
        P(None, None, "gx", "gy", "gz"),
        P("gx", "gy", "gz"),
        P(),
        P(),
    )
    sizes = tuple(mesh.shape[axis] for axis in AXES)
    return jax.shard_map(
        functools.partial(on_device, sizes),
        mesh=mesh,
        in_specs=placed,
        out_specs=(P(None, "gx", "gy", "gz"), P(None, "gx", "gy", "gz")),
        check_vma=False,
    )
```

```python
import functools

import jax
import jax.numpy as jnp
from jax import lax
from jax.experimental import pallas as pl
from jax.experimental.pallas import tpu as pltpu
from jax.sharding import PartitionSpec as P

penalty = 0.15
epsilon = 1e-06
highest = lax.Precision.HIGHEST
AXES = ("gx", "gy", "gz")
MESH = pl.DeviceIdType.MESH
LANES = 128
SUBLANES = 8
EXCHANGES = 3


def offsets(sizes):
    return [
        (a, b, c)
        for a in range(sizes[0])
        for b in range(sizes[1])
        for c in range(sizes[2])
        if a or b or c
    ]


def iota(shape, dim):
    return lax.broadcasted_iota(jnp.int32, shape, dim)


def line_matrix(stiffness, row, col):
    points = stiffness.shape[0]
    size = row.shape[0]
    picks = jnp.where(row[:, :1] % points == iota((size, points), 1), 1.0, 0.0)
    spread = jnp.dot(picks, stiffness, precision=highest, preferred_element_type=jnp.float32)
    spread = lax.dot_general(
        spread, picks, (((1,), (1,)), ((), ())), precision=highest,
        preferred_element_type=jnp.float32,
    )
    inside = jnp.where(row // points == col // points, spread, 0.0)
    first, last = row % points == 0, row % points == points - 1
    ends = jnp.where(first, penalty, 0.0) + jnp.where(last, penalty, 0.0)
    inside = inside + jnp.where(row == col, ends, 0.0)
    inside = inside - jnp.where((col == row + 1) & last, penalty, 0.0)
    return inside - jnp.where((col == row - 1) & first, penalty, 0.0)


def kernel(
    sizes, total_points,
    rhs_any, basis_any, inertia_any, helm, stiffness_any,
    sol, new,
    rhs, basis, inertia, stiffness, load_sem,
    wide, x0, r0, q, mat_z, mat_xy,
    face_y, face_z, ghost_x, ghost_y, ghost_z,
    row1, rows2, got1, got2,
    halo_send, halo_recv, send1, recv1, send2, recv2,
):
    solves, keep, size_x, size_y, size_z = basis.shape
    here = tuple(lax.axis_index(axis) for axis in AXES)
    moves = offsets(sizes)
    unrolled = len(moves) <= 64
    inverse = 1.0 / total_points

    def partner(move):
        return {
            axis: lax.rem(here[d] + move[d], sizes[d]) for d, axis in enumerate(AXES)
        }

    def for_all(act):
        if unrolled:
            for slot, move in enumerate(moves):
                act(slot, partner(move))
        else:
            def step(index, carry):
                away = index + 1
                move = (
                    away // (sizes[1] * sizes[2]),
                    (away // sizes[2]) % sizes[1],
                    away % sizes[2],
                )
                act(index, partner(move))
                return carry
            lax.fori_loop(0, len(moves), step, 0)

    loads = [
        pltpu.make_async_copy(source, target, load_sem.at[at])
        for at, (source, target) in enumerate(
            (
                (rhs_any, rhs), (basis_any, basis),
                (inertia_any, inertia), (stiffness_any, stiffness),
            )
        )
    ]
    for load in loads:
        load.start()
    ghost_x[...] = jnp.zeros_like(ghost_x)
    ghost_y[...] = jnp.zeros_like(ghost_y)
    ghost_z[...] = jnp.zeros_like(ghost_z)
    barrier = pltpu.get_barrier_semaphore()
    for_all(
        lambda slot, target: pl.semaphore_signal(
            barrier, inc=1, device_id=target, device_id_type=MESH
        )
    )

    def row_of(parts):
        stack = jnp.concatenate([jnp.sum(part, axis=0, keepdims=True) for part in parts], axis=0)
        if len(parts) < LANES:
            stack = jnp.concatenate(
                [stack, jnp.zeros((LANES - len(parts), stack.shape[1]), jnp.float32)], axis=0
            )
        return lax.dot_general(
            jnp.ones((SUBLANES, stack.shape[1]), jnp.float32), stack,
            (((1,), (1,)), ((), ())), precision=highest, preferred_element_type=jnp.float32,
        )[:1]

    def inner(a, b):
        return jnp.sum(a * b, axis=0)

    def splat(row, lane):
        return jnp.broadcast_to(row[:, lane:lane + 1], (size_y, size_z))

    def send_all(source, got, send, recv):
        def act(slot, target):
            pltpu.make_async_remote_copy(
                src_ref=source, dst_ref=got.at[slot], send_sem=send, recv_sem=recv,
                device_id=target, device_id_type=MESH,
            ).start()
        for_all(act)

    def take_all(got, send, recv):
        pltpu.make_async_copy(got, got, send).wait()
        pltpu.make_async_copy(got, got, recv).wait()

    parts = []
    for load in loads:
        load.wait()
    for s in range(solves):
        for k in range(keep):
            stored = basis[s, k].astype(jnp.float32)
            wide[s, k] = stored
            parts.append(inner(stored, rhs[s]))
    row1[...] = row_of(parts)
    pl.semaphore_wait(barrier, len(moves))
    send_all(row1, got1, send1, recv1)

    row, col = iota((size_z, size_z), 0), iota((size_z, size_z), 1)
    mat_z[...] = line_matrix(stiffness[...], row, col)
    area = size_x * size_y
    row, col = iota((area, area), 0), iota((area, area), 1)
    row_x, col_x, row_y, col_y = row // size_y, col // size_y, row % size_y, col % size_y
    mat_xy[...] = jnp.where(
        row_y == col_y, line_matrix(stiffness[...], row_x, col_x), 0.0
    ) + jnp.where(row_x == col_x, line_matrix(stiffness[...], row_y, col_y), 0.0)
    pairs = [(k, l) for k in range(keep) for l in range(k, keep)]
    gram = [inner(wide[s, k], wide[s, l]) for s in range(solves) for k, l in pairs]
    rows2[1:2] = row_of(gram[:LANES])
    gram_rest = gram[LANES:]

    lane = iota((size_y, size_z), 1)
    sub = iota((size_y, size_z), 0)

    def exchange(index, field):
        for s in range(solves):
            for side, pos in ((0, 0), (1, size_y - 1)):
                face_y[index, side, s] = jnp.concatenate(
                    [field[s, x, pos:pos + 1, :] for x in range(size_x)], axis=0
                )
        for side, pos in ((0, 0), (1, size_z - 1)):
            pack = jnp.zeros((size_y, size_z), jnp.float32)
            for s in range(solves):
                for x in range(size_x):
                    column = jnp.broadcast_to(field[s, x, :, pos:pos + 1], (size_y, size_z))
                    pack = jnp.where(lane == s * size_x + x, column, pack)
            face_z[index, side] = pack

        def each(act):
            for d, axis in enumerate(AXES):
                if sizes[d] == 1:
                    continue
                for side, step in ((0, -1), (1, 1)):
                    if d == 0:
                        source = field.at[:, 0 if side == 0 else size_x - 1]
                        target = ghost_x.at[index, 1 - side]
                    elif d == 1:
                        source, target = face_y.at[index, side], ghost_y.at[index, 1 - side]
                    else:
                        source, target = face_z.at[index, side], ghost_z.at[index, 1 - side]
                    sends = here[d] > 0 if side == 0 else here[d] < sizes[d] - 1
                    takes = here[d] < sizes[d] - 1 if side == 0 else here[d] > 0
                    copy = pltpu.make_async_remote_copy(
                        src_ref=source, dst_ref=target,
                        send_sem=halo_send.at[index, 2 * d + side],
                        recv_sem=halo_recv.at[index, 2 * d + side],
                        device_id={axis: jnp.clip(here[d] + step, 0, sizes[d] - 1)},
                        device_id_type=MESH,
                    )
                    act(copy, sends, takes)

        def start(copy, sends, takes):
            @pl.when(sends)
            def _():
                copy.start()

        def finish(copy, sends, takes):
            @pl.when(takes)
            def _():
                copy.wait_recv()

            @pl.when(sends)
            def _():
                copy.wait_send()

        each(start)
        return lambda: each(finish)

    def local(field, s):
        flat = field[s].reshape(area, size_z)
        along_z = jnp.dot(flat, mat_z[...], precision=highest, preferred_element_type=jnp.float32)
        along_xy = jnp.dot(mat_xy[...], flat, precision=highest, preferred_element_type=jnp.float32)
        out = (along_z + along_xy).reshape(size_x, size_y, size_z)
        return out + helm[s] * inertia[...] * field[s]

    def coupled(index, s):
        low_z, high_z = ghost_z[index, 0], ghost_z[index, 1]
        planes = []
        for x in range(size_x):
            spot = s * size_x + x
            plane = jnp.where(lane == 0, jnp.broadcast_to(low_z[:, spot:spot + 1], lane.shape), 0.0)
            plane = jnp.where(
                lane == size_z - 1, jnp.broadcast_to(high_z[:, spot:spot + 1], lane.shape), plane
            )
            plane = plane + jnp.where(
                sub == 0, jnp.broadcast_to(ghost_y[index, 0, s, x:x + 1, :], lane.shape), 0.0
            )
            plane = plane + jnp.where(
                sub == size_y - 1,
                jnp.broadcast_to(ghost_y[index, 1, s, x:x + 1, :], lane.shape), 0.0,
            )
            if x == 0:
                plane = plane + ghost_x[index, 0, s]
            if x == size_x - 1:
                plane = plane + ghost_x[index, 1, s]
            planes.append(plane)
        return penalty * jnp.stack(planes)

    take_all(got1, send1, recv1)
    coefs = (row1[...] + jnp.sum(got1[...], axis=0)) * inverse
    for s in range(solves):
        total = jnp.zeros((size_x, size_y, size_z), jnp.float32)
        for k in range(keep):
            total = total + splat(coefs, s * keep + k)[None] * wide[s, k]
        x0[s] = total
    finish = exchange(0, x0)
    for s in range(solves):
        r0[s] = rhs[s] - local(x0, s)
    finish()
    for s in range(solves):
        r0[s] = r0[s] + coupled(0, s)
    finish = exchange(1, r0)
    for s in range(solves):
        q[s] = local(r0, s)
    with_r = [inner(wide[s, k], r0[s]) for s in range(solves) for k in range(keep)]
    finish()
    for s in range(solves):
        q[s] = q[s] - coupled(1, s)
    finish = exchange(2, q)
    with_q = [inner(wide[s, k], q[s]) for s in range(solves) for k in range(keep)]
    moments = []
    for s in range(solves):
        moments.append(
            [inner(r0[s], r0[s]), inner(r0[s], q[s]), inner(q[s], q[s]), inner(q[s], local(q, s))]
        )
    finish()
    for s in range(solves):
        moments[s][3] = moments[s][3] - inner(q[s], coupled(2, s))
    flat_moments = [moments[s][j] for s in range(solves) for j in range(4)]
    rows2[0:1] = row_of(with_r + with_q + flat_moments + gram_rest)
    send_all(rows2, got2, send2, recv2)
    take_all(got2, send2, recv2)
    sums = (rows2[...] + jnp.sum(got2[...], axis=0)) * inverse
    main, other = sums[0:1], sums[1:2]
    at_q, at_m = solves * keep, 2 * solves * keep
    at_rest = at_m + 4 * solves

    for s in range(solves):
        coef = [splat(coefs, s * keep + k) for k in range(keep)]
        by_r = [splat(main, s * keep + k) for k in range(keep)]
        by_q = [splat(main, at_q + s * keep + k) for k in range(keep)]
        m0, m1, m2, m3 = (splat(main, at_m + 4 * s + j) for j in range(4))
        table = {}
        for at, (k, l) in enumerate(pairs):
            spot = s * len(pairs) + at
            value = splat(other, spot) if spot < LANES else splat(main, at_rest + spot - LANES)
            table[k, l] = table[l, k] = value
        first = m0 / m1
        middle = m2 / m1
        across = m3 / m1 - middle * middle
        flat = across <= 1e-6 * middle * middle
        second = jnp.where(flat, 0.0, (1.0 - first * middle) / jnp.where(flat, 1.0, across))
        on_q = second
        on_r = first - second * middle
        moved = [
            functools.reduce(lambda a, b: a + b, [table[k, l] * coef[l] for l in range(keep)])
            for k in range(keep)
        ]
        weight = [moved[k] + on_r * by_r[k] + on_q * by_q[k] for k in range(keep)]
        square = on_r * on_r * m0 + 2.0 * on_r * on_q * m1 + on_q * on_q * m2
        mixed = jnp.zeros_like(square)
        for k in range(keep):
            square = square + coef[k] * (2.0 * weight[k] - moved[k])
            pulled = functools.reduce(
                lambda a, b: a + b, [table[k, l] * weight[l] for l in range(keep)]
            )
            mixed = mixed + weight[k] * (pulled - 2.0 * weight[k])
        scale = lax.rsqrt(square + mixed + epsilon)
        answer = x0[s] + on_r[None] * r0[s] + on_q[None] * q[s]
        sol[s] = answer
        for k in range(keep):
            answer = answer - weight[k][None] * wide[s, k]
        new[s] = answer * scale[None]


def write(sol_in, new_in, sol, new):
    sol[...] = sol_in[...]
    new[...] = new_in[...].astype(jnp.bfloat16)


def on_device(sizes, rhs, basis, inertia, helm, stiffness):
    solves, size_x, size_y, size_z = rhs.shape
    total_points = float(rhs[0].size * sizes[0] * sizes[1] * sizes[2])
    others = sizes[0] * sizes[1] * sizes[2] - 1
    field = pltpu.VMEM(rhs.shape, jnp.float32)
    vmem = pl.BlockSpec(memory_space=pltpu.VMEM)
    smem = pl.BlockSpec(memory_space=pltpu.SMEM)
    area = size_x * size_y
    faces = (EXCHANGES, 2, solves)
    anywhere = pl.BlockSpec(memory_space=pl.ANY)
    held = pl.pallas_call(
        functools.partial(kernel, sizes, total_points),
        out_shape=(field, field),
        in_specs=[anywhere, anywhere, anywhere, smem, anywhere],
        out_specs=(vmem, vmem),
        scratch_shapes=[
            field,
            pltpu.VMEM(basis.shape, basis.dtype),
            pltpu.VMEM(inertia.shape, inertia.dtype),
            pltpu.VMEM(stiffness.shape, stiffness.dtype),
            pltpu.SemaphoreType.DMA((4,)),
            pltpu.VMEM(basis.shape, jnp.float32),
            field, field, field,
            pltpu.VMEM((size_z, size_z), jnp.float32),
            pltpu.VMEM((area, area), jnp.float32),
            pltpu.VMEM((*faces, size_x, size_z), jnp.float32),
            pltpu.VMEM((EXCHANGES, 2, size_y, size_z), jnp.float32),
            pltpu.VMEM((*faces, size_y, size_z), jnp.float32),
            pltpu.VMEM((*faces, size_x, size_z), jnp.float32),
            pltpu.VMEM((EXCHANGES, 2, size_y, size_z), jnp.float32),
            pltpu.VMEM((1, LANES), jnp.float32),
            pltpu.VMEM((2, LANES), jnp.float32),
            pltpu.VMEM((others, 1, LANES), jnp.float32),
            pltpu.VMEM((others, 2, LANES), jnp.float32),
            pltpu.SemaphoreType.DMA((EXCHANGES, 6)),
            pltpu.SemaphoreType.DMA((EXCHANGES, 6)),
            pltpu.SemaphoreType.DMA,
            pltpu.SemaphoreType.DMA,
            pltpu.SemaphoreType.DMA,
            pltpu.SemaphoreType.DMA,
        ],
        compiler_params=pltpu.CompilerParams(collective_id=0, has_side_effects=True),
    )(rhs, basis, inertia, helm, stiffness)
    return pl.pallas_call(
        write,
        out_shape=(
            jax.ShapeDtypeStruct(rhs.shape, jnp.float32),
            jax.ShapeDtypeStruct(rhs.shape, jnp.bfloat16),
        ),
        in_specs=[vmem, vmem],
        out_specs=(vmem, vmem),
    )(*(pltpu.with_memory_space_constraint(part, pltpu.VMEM) for part in held))


def solution(mesh):
    placed = (
        P(None, "gx", "gy", "gz"),
        P(None, None, "gx", "gy", "gz"),
        P("gx", "gy", "gz"),
        P(),
        P(),
    )
    sizes = tuple(mesh.shape[axis] for axis in AXES)
    return jax.shard_map(
        functools.partial(on_device, sizes),
        mesh=mesh,
        in_specs=placed,
        out_specs=(P(None, "gx", "gy", "gz"), P(None, "gx", "gy", "gz")),
        check_vma=False,
    )
```

```python
import functools

import jax
import jax.numpy as jnp
from jax import lax
from jax.experimental import pallas as pl
from jax.experimental.pallas import tpu as pltpu
from jax.sharding import PartitionSpec as P

penalty = 0.15
epsilon = 1e-06
highest = lax.Precision.HIGHEST
AXES = ("gx", "gy", "gz")
MESH = pl.DeviceIdType.MESH
LANES = 128
SUBLANES = 8
EXCHANGES = 2


def offsets(sizes):
    return [
        (a, b, c)
        for a in range(sizes[0])
        for b in range(sizes[1])
        for c in range(sizes[2])
        if a or b or c
    ]


def iota(shape, dim):
    return lax.broadcasted_iota(jnp.int32, shape, dim)


def line_matrix(stiffness, row, col):
    points = stiffness.shape[0]
    size = row.shape[0]
    picks = jnp.where(row[:, :1] % points == iota((size, points), 1), 1.0, 0.0)
    spread = jnp.dot(picks, stiffness, precision=highest, preferred_element_type=jnp.float32)
    spread = lax.dot_general(
        spread, picks, (((1,), (1,)), ((), ())), precision=highest,
        preferred_element_type=jnp.float32,
    )
    inside = jnp.where(row // points == col // points, spread, 0.0)
    first, last = row % points == 0, row % points == points - 1
    ends = jnp.where(first, penalty, 0.0) + jnp.where(last, penalty, 0.0)
    inside = inside + jnp.where(row == col, ends, 0.0)
    inside = inside - jnp.where((col == row + 1) & last, penalty, 0.0)
    return inside - jnp.where((col == row - 1) & first, penalty, 0.0)


def kernel(
    sizes, total_points,
    rhs_any, basis_any, inertia_any, helm, stiffness_any,
    sol, new,
    rhs, basis, inertia, stiffness, load_sem,
    wide, x0, r0, q, mat_z, mat_xy,
    face_y, face_z, ghost_x, ghost_y, ghost_z,
    many_face_y, many_face_z, many_x, many_y, many_z,
    row1, rows2, got1, got2,
    halo_send, halo_recv, send1, recv1, send2, recv2,
):
    solves, keep, size_x, size_y, size_z = basis.shape
    here = tuple(lax.axis_index(axis) for axis in AXES)
    moves = offsets(sizes)
    unrolled = len(moves) <= 64
    inverse = 1.0 / total_points

    def partner(move):
        return {
            axis: lax.rem(here[d] + move[d], sizes[d]) for d, axis in enumerate(AXES)
        }

    def for_all(act):
        if unrolled:
            for slot, move in enumerate(moves):
                act(slot, partner(move))
        else:
            def step(index, carry):
                away = index + 1
                move = (
                    away // (sizes[1] * sizes[2]),
                    (away // sizes[2]) % sizes[1],
                    away % sizes[2],
                )
                act(index, partner(move))
                return carry
            lax.fori_loop(0, len(moves), step, 0)

    loads = [
        pltpu.make_async_copy(source, target, load_sem.at[at])
        for at, (source, target) in enumerate(
            (
                (rhs_any, rhs), (basis_any, basis),
                (inertia_any, inertia), (stiffness_any, stiffness),
            )
        )
    ]
    for load in loads:
        load.start()
    for ghost in (ghost_x, ghost_y, ghost_z, many_x, many_y, many_z):
        ghost[...] = jnp.zeros_like(ghost)
    barrier = pltpu.get_barrier_semaphore()
    for_all(
        lambda slot, target: pl.semaphore_signal(
            barrier, inc=1, device_id=target, device_id_type=MESH
        )
    )

    def row_of(parts):
        stack = jnp.concatenate([jnp.sum(part, axis=0, keepdims=True) for part in parts], axis=0)
        if len(parts) < LANES:
            stack = jnp.concatenate(
                [stack, jnp.zeros((LANES - len(parts), stack.shape[1]), jnp.float32)], axis=0
            )
        return lax.dot_general(
            jnp.ones((SUBLANES, stack.shape[1]), jnp.float32), stack,
            (((1,), (1,)), ((), ())), precision=highest, preferred_element_type=jnp.float32,
        )[:1]

    def inner(a, b):
        return jnp.sum(a * b, axis=0)

    def splat(row, lane):
        return jnp.broadcast_to(row[:, lane:lane + 1], (size_y, size_z))

    def send_all(source, got, send, recv):
        def act(slot, target):
            pltpu.make_async_remote_copy(
                src_ref=source, dst_ref=got.at[slot], send_sem=send, recv_sem=recv,
                device_id=target, device_id_type=MESH,
            ).start()
        for_all(act)

    def take_all(got, send, recv):
        pltpu.make_async_copy(got, got, send).wait()
        pltpu.make_async_copy(got, got, recv).wait()

    lane = iota((size_y, size_z), 1)
    sub = iota((size_y, size_z), 0)

    def column_pack(plane_of, pos):
        pack = jnp.zeros((size_y, size_z), jnp.float32)
        for s in range(solves):
            for x in range(size_x):
                column = jnp.broadcast_to(plane_of(s, x)[:, pos:pos + 1], (size_y, size_z))
                pack = jnp.where(lane == s * size_x + x, column, pack)
        return pack

    def trade(index, source, target):
        def each(act):
            for d, axis in enumerate(AXES):
                if sizes[d] == 1:
                    continue
                for side, step in ((0, -1), (1, 1)):
                    sends = here[d] > 0 if side == 0 else here[d] < sizes[d] - 1
                    takes = here[d] < sizes[d] - 1 if side == 0 else here[d] > 0
                    copy = pltpu.make_async_remote_copy(
                        src_ref=source(d, side), dst_ref=target(d, 1 - side),
                        send_sem=halo_send.at[index, 2 * d + side],
                        recv_sem=halo_recv.at[index, 2 * d + side],
                        device_id={axis: jnp.clip(here[d] + step, 0, sizes[d] - 1)},
                        device_id_type=MESH,
                    )
                    act(copy, sends, takes)

        def start(copy, sends, takes):
            @pl.when(sends)
            def _():
                copy.start()

        def finish(copy, sends, takes):
            @pl.when(takes)
            def _():
                copy.wait_recv()

            @pl.when(sends)
            def _():
                copy.wait_send()

        each(start)
        return lambda: each(finish)

    parts = []
    for load in loads:
        load.wait()
    for s in range(solves):
        for k in range(keep):
            stored = basis[s, k].astype(jnp.float32)
            wide[s, k] = stored
            parts.append(inner(stored, rhs[s]))
    row1[...] = row_of(parts)
    ends_x, ends_y, ends_z = ((0, size - 1) for size in (size_x, size_y, size_z))
    for k in range(keep):
        for side in (0, 1):
            for s in range(solves):
                many_face_y[side, s, k] = jnp.concatenate(
                    [wide[s, k, x, ends_y[side]:ends_y[side] + 1, :] for x in range(size_x)],
                    axis=0,
                )
            many_face_z[side, k] = column_pack(lambda s, x: wide[s, k, x], ends_z[side])
    pl.semaphore_wait(barrier, len(moves))
    send_all(row1, got1, send1, recv1)
    finish_many = trade(
        0,
        lambda d, side: (
            wide.at[:, :, ends_x[side]], many_face_y.at[side], many_face_z.at[side]
        )[d],
        lambda d, side: (many_x, many_y, many_z)[d].at[side],
    )

    row, col = iota((size_z, size_z), 0), iota((size_z, size_z), 1)
    mat_z[...] = line_matrix(stiffness[...], row, col)
    area = size_x * size_y
    row, col = iota((area, area), 0), iota((area, area), 1)
    row_x, col_x, row_y, col_y = row // size_y, col // size_y, row % size_y, col % size_y
    mat_xy[...] = jnp.where(
        row_y == col_y, line_matrix(stiffness[...], row_x, col_x), 0.0
    ) + jnp.where(row_x == col_x, line_matrix(stiffness[...], row_y, col_y), 0.0)
    pairs = [(k, l) for k in range(keep) for l in range(k, keep)]
    gram = [inner(wide[s, k], wide[s, l]) for s in range(solves) for k, l in pairs]
    rows2[1:2] = row_of(gram[:LANES])
    gram_rest = gram[LANES:]

    def exchange(index, field):
        for s in range(solves):
            for side, pos in ((0, 0), (1, size_y - 1)):
                face_y[index, side, s] = jnp.concatenate(
                    [field[s, x, pos:pos + 1, :] for x in range(size_x)], axis=0
                )
        for side, pos in ((0, 0), (1, size_z - 1)):
            face_z[index, side] = column_pack(lambda s, x: field[s, x], pos)
        return trade(
            1 + index,
            lambda d, side: (
                field.at[:, ends_x[side]], face_y.at[index, side], face_z.at[index, side]
            )[d],
            lambda d, side: (ghost_x, ghost_y, ghost_z)[d].at[index, side],
        )

    def local(field, s):
        flat = field[s].reshape(area, size_z)
        along_z = jnp.dot(flat, mat_z[...], precision=highest, preferred_element_type=jnp.float32)
        along_xy = jnp.dot(mat_xy[...], flat, precision=highest, preferred_element_type=jnp.float32)
        out = (along_z + along_xy).reshape(size_x, size_y, size_z)
        return out + helm[s] * inertia[...] * field[s]

    def coupled(s, ghost_x, ghost_y, ghost_z):
        low_z, high_z = ghost_z(0), ghost_z(1)
        low_y, high_y = ghost_y(0, s), ghost_y(1, s)
        planes = []
        for x in range(size_x):
            spot = s * size_x + x
            plane = jnp.where(lane == 0, jnp.broadcast_to(low_z[:, spot:spot + 1], lane.shape), 0.0)
            plane = jnp.where(
                lane == size_z - 1, jnp.broadcast_to(high_z[:, spot:spot + 1], lane.shape), plane
            )
            plane = plane + jnp.where(
                sub == 0, jnp.broadcast_to(low_y[x:x + 1, :], lane.shape), 0.0
            )
            plane = plane + jnp.where(
                sub == size_y - 1,
                jnp.broadcast_to(high_y[x:x + 1, :], lane.shape), 0.0,
            )
            if x == 0:
                plane = plane + ghost_x(0, s)
            if x == size_x - 1:
                plane = plane + ghost_x(1, s)
            planes.append(plane)
        return penalty * jnp.stack(planes)

    def received(index, s):
        return coupled(
            s,
            lambda side, at: ghost_x[index, side, at],
            lambda side, at: ghost_y[index, side, at],
            lambda side: ghost_z[index, side],
        )

    take_all(got1, send1, recv1)
    coefs = (row1[...] + jnp.sum(got1[...], axis=0)) * inverse
    splats = [[splat(coefs, s * keep + k) for k in range(keep)] for s in range(solves)]
    for s in range(solves):
        total = jnp.zeros((size_x, size_y, size_z), jnp.float32)
        for k in range(keep):
            total = total + splats[s][k][None] * wide[s, k]
        x0[s] = total
    for s in range(solves):
        r0[s] = rhs[s] - local(x0, s)
    by_lane = []
    for k in range(keep):
        mixed = jnp.zeros((size_y, size_z), jnp.float32)
        for s in range(solves):
            mixed = jnp.where(lane // size_x == s, splats[s][k], mixed)
        by_lane.append(mixed)
    finish_many()

    def combined(values):
        return functools.reduce(lambda a, b: a + b, values)

    both_z = [
        combined([by_lane[k] * many_z[side, k] for k in range(keep)]) for side in (0, 1)
    ]
    for s in range(solves):
        r0[s] = r0[s] + coupled(
            s,
            lambda side, at: combined([splats[at][k] * many_x[side, at, k] for k in range(keep)]),
            lambda side, at: combined([splats[at][k] * many_y[side, at, k] for k in range(keep)]),
            lambda side: both_z[side],
        )
    finish = exchange(0, r0)
    for s in range(solves):
        q[s] = local(r0, s)
    with_r = [inner(wide[s, k], r0[s]) for s in range(solves) for k in range(keep)]
    finish()
    for s in range(solves):
        q[s] = q[s] - received(0, s)
    finish = exchange(1, q)
    with_q = [inner(wide[s, k], q[s]) for s in range(solves) for k in range(keep)]
    moments = []
    for s in range(solves):
        moments.append(
            [inner(r0[s], r0[s]), inner(r0[s], q[s]), inner(q[s], q[s]), inner(q[s], local(q, s))]
        )
    finish()
    for s in range(solves):
        moments[s][3] = moments[s][3] - inner(q[s], received(1, s))
    flat_moments = [moments[s][j] for s in range(solves) for j in range(4)]
    rows2[0:1] = row_of(with_r + with_q + flat_moments + gram_rest)
    send_all(rows2, got2, send2, recv2)
    take_all(got2, send2, recv2)
    sums = (rows2[...] + jnp.sum(got2[...], axis=0)) * inverse
    main, other = sums[0:1], sums[1:2]
    at_q, at_m = solves * keep, 2 * solves * keep
    at_rest = at_m + 4 * solves

    for s in range(solves):
        coef = [splat(coefs, s * keep + k) for k in range(keep)]
        by_r = [splat(main, s * keep + k) for k in range(keep)]
        by_q = [splat(main, at_q + s * keep + k) for k in range(keep)]
        m0, m1, m2, m3 = (splat(main, at_m + 4 * s + j) for j in range(4))
        table = {}
        for at, (k, l) in enumerate(pairs):
            spot = s * len(pairs) + at
            value = splat(other, spot) if spot < LANES else splat(main, at_rest + spot - LANES)
            table[k, l] = table[l, k] = value
        first = m0 / m1
        middle = m2 / m1
        across = m3 / m1 - middle * middle
        flat = across <= 1e-6 * middle * middle
        second = jnp.where(flat, 0.0, (1.0 - first * middle) / jnp.where(flat, 1.0, across))
        on_q = second
        on_r = first - second * middle
        moved = [
            functools.reduce(lambda a, b: a + b, [table[k, l] * coef[l] for l in range(keep)])
            for k in range(keep)
        ]
        weight = [moved[k] + on_r * by_r[k] + on_q * by_q[k] for k in range(keep)]
        square = on_r * on_r * m0 + 2.0 * on_r * on_q * m1 + on_q * on_q * m2
        mixed = jnp.zeros_like(square)
        for k in range(keep):
            square = square + coef[k] * (2.0 * weight[k] - moved[k])
            pulled = functools.reduce(
                lambda a, b: a + b, [table[k, l] * weight[l] for l in range(keep)]
            )
            mixed = mixed + weight[k] * (pulled - 2.0 * weight[k])
        scale = lax.rsqrt(square + mixed + epsilon)
        answer = x0[s] + on_r[None] * r0[s] + on_q[None] * q[s]
        sol[s] = answer
        for k in range(keep):
            answer = answer - weight[k][None] * wide[s, k]
        new[s] = answer * scale[None]


def write(sol_in, new_in, sol, new):
    sol[...] = sol_in[...]
    new[...] = new_in[...].astype(jnp.bfloat16)


def on_device(sizes, rhs, basis, inertia, helm, stiffness):
    solves, size_x, size_y, size_z = rhs.shape
    keep = basis.shape[1]
    total_points = float(rhs[0].size * sizes[0] * sizes[1] * sizes[2])
    others = sizes[0] * sizes[1] * sizes[2] - 1
    field = pltpu.VMEM(rhs.shape, jnp.float32)
    vmem = pl.BlockSpec(memory_space=pltpu.VMEM)
    smem = pl.BlockSpec(memory_space=pltpu.SMEM)
    area = size_x * size_y
    faces = (EXCHANGES, 2, solves)
    anywhere = pl.BlockSpec(memory_space=pl.ANY)
    held = pl.pallas_call(
        functools.partial(kernel, sizes, total_points),
        out_shape=(field, field),
        in_specs=[anywhere, anywhere, anywhere, smem, anywhere],
        out_specs=(vmem, vmem),
        scratch_shapes=[
            field,
            pltpu.VMEM(basis.shape, basis.dtype),
            pltpu.VMEM(inertia.shape, inertia.dtype),
            pltpu.VMEM(stiffness.shape, stiffness.dtype),
            pltpu.SemaphoreType.DMA((4,)),
            pltpu.VMEM(basis.shape, jnp.float32),
            field, field, field,
            pltpu.VMEM((size_z, size_z), jnp.float32),
            pltpu.VMEM((area, area), jnp.float32),
            pltpu.VMEM((*faces, size_x, size_z), jnp.float32),
            pltpu.VMEM((EXCHANGES, 2, size_y, size_z), jnp.float32),
            pltpu.VMEM((*faces, size_y, size_z), jnp.float32),
            pltpu.VMEM((*faces, size_x, size_z), jnp.float32),
            pltpu.VMEM((EXCHANGES, 2, size_y, size_z), jnp.float32),
            pltpu.VMEM((2, solves, keep, size_x, size_z), jnp.float32),
            pltpu.VMEM((2, keep, size_y, size_z), jnp.float32),
            pltpu.VMEM((2, solves, keep, size_y, size_z), jnp.float32),
            pltpu.VMEM((2, solves, keep, size_x, size_z), jnp.float32),
            pltpu.VMEM((2, keep, size_y, size_z), jnp.float32),
            pltpu.VMEM((1, LANES), jnp.float32),
            pltpu.VMEM((2, LANES), jnp.float32),
            pltpu.VMEM((others, 1, LANES), jnp.float32),
            pltpu.VMEM((others, 2, LANES), jnp.float32),
            pltpu.SemaphoreType.DMA((1 + EXCHANGES, 6)),
            pltpu.SemaphoreType.DMA((1 + EXCHANGES, 6)),
            pltpu.SemaphoreType.DMA,
            pltpu.SemaphoreType.DMA,
            pltpu.SemaphoreType.DMA,
            pltpu.SemaphoreType.DMA,
        ],
        compiler_params=pltpu.CompilerParams(collective_id=0, has_side_effects=True),
    )(rhs, basis, inertia, helm, stiffness)
    return pl.pallas_call(
        write,
        out_shape=(
            jax.ShapeDtypeStruct(rhs.shape, jnp.float32),
            jax.ShapeDtypeStruct(rhs.shape, jnp.bfloat16),
        ),
        in_specs=[vmem, vmem],
        out_specs=(vmem, vmem),
    )(*(pltpu.with_memory_space_constraint(part, pltpu.VMEM) for part in held))


def solution(mesh):
    placed = (
        P(None, "gx", "gy", "gz"),
        P(None, None, "gx", "gy", "gz"),
        P("gx", "gy", "gz"),
        P(),
        P(),
    )
    sizes = tuple(mesh.shape[axis] for axis in AXES)
    return jax.shard_map(
        functools.partial(on_device, sizes),
        mesh=mesh,
        in_specs=placed,
        out_specs=(P(None, "gx", "gy", "gz"), P(None, "gx", "gy", "gz")),
        check_vma=False,
    )
```

```python
import functools

import jax
import jax.numpy as jnp
from jax import lax
from jax.experimental import pallas as pl
from jax.experimental.pallas import tpu as pltpu
from jax.sharding import PartitionSpec as P

penalty = 0.15
epsilon = 1e-06
highest = lax.Precision.HIGHEST
AXES = ("gx", "gy", "gz")
MESH = pl.DeviceIdType.MESH
LANES = 128
SUBLANES = 8
EXCHANGES = 2


def offsets(sizes):
    return [
        (a, b, c)
        for a in range(sizes[0])
        for b in range(sizes[1])
        for c in range(sizes[2])
        if a or b or c
    ]


def iota(shape, dim):
    return lax.broadcasted_iota(jnp.int32, shape, dim)


def line_matrix(stiffness, row, col):
    points = stiffness.shape[0]
    size = row.shape[0]
    picks = jnp.where(row[:, :1] % points == iota((size, points), 1), 1.0, 0.0)
    spread = jnp.dot(picks, stiffness, precision=highest, preferred_element_type=jnp.float32)
    spread = lax.dot_general(
        spread, picks, (((1,), (1,)), ((), ())), precision=highest,
        preferred_element_type=jnp.float32,
    )
    inside = jnp.where(row // points == col // points, spread, 0.0)
    first, last = row % points == 0, row % points == points - 1
    ends = jnp.where(first, penalty, 0.0) + jnp.where(last, penalty, 0.0)
    inside = inside + jnp.where(row == col, ends, 0.0)
    inside = inside - jnp.where((col == row + 1) & last, penalty, 0.0)
    return inside - jnp.where((col == row - 1) & first, penalty, 0.0)


def halves(values):
    high = values.astype(jnp.bfloat16)
    return high, (values - high.astype(jnp.float32)).astype(jnp.bfloat16)


def kernel(
    sizes, total_points,
    rhs_any, basis_any, inertia_any, helm, stiffness_any,
    sol, new,
    rhs, basis, inertia, stiffness, load_sem,
    wide, x0, r0, q, mat_z, mat_xy,
    face_y, face_z, ghost_x, ghost_y, ghost_z,
    many_face_y, many_face_z, many_x, many_y, many_z,
    row1, rows2, got1, got2,
    halo_send, halo_recv, send1, recv1, send2, recv2,
):
    solves, keep, size_x, size_y, size_z = basis.shape
    here = tuple(lax.axis_index(axis) for axis in AXES)
    moves = offsets(sizes)
    unrolled = len(moves) <= 64
    inverse = 1.0 / total_points
    at_q, at_m = solves * keep, 2 * solves * keep
    at_rest = at_m + 4 * solves

    def partner(move):
        return {
            axis: lax.rem(here[d] + move[d], sizes[d]) for d, axis in enumerate(AXES)
        }

    def for_all(act):
        if unrolled:
            for slot, move in enumerate(moves):
                act(slot, partner(move))
        else:
            def step(index, carry):
                away = index + 1
                move = (
                    away // (sizes[1] * sizes[2]),
                    (away // sizes[2]) % sizes[1],
                    away % sizes[2],
                )
                act(index, partner(move))
                return carry
            lax.fori_loop(0, len(moves), step, 0)

    loads = [
        pltpu.make_async_copy(source, target, load_sem.at[at])
        for at, (source, target) in enumerate(
            (
                (rhs_any, rhs), (basis_any, basis),
                (inertia_any, inertia), (stiffness_any, stiffness),
            )
        )
    ]
    for load in loads:
        load.start()
    for ghost in (ghost_x, ghost_y, ghost_z, many_x, many_y, many_z):
        ghost[...] = jnp.zeros_like(ghost)
    barrier = pltpu.get_barrier_semaphore()
    for_all(
        lambda slot, target: pl.semaphore_signal(
            barrier, inc=1, device_id=target, device_id_type=MESH
        )
    )

    def row_of(parts):
        stack = jnp.concatenate([jnp.sum(part, axis=0, keepdims=True) for part in parts], axis=0)
        if len(parts) < LANES:
            stack = jnp.concatenate(
                [stack, jnp.zeros((LANES - len(parts), stack.shape[1]), jnp.float32)], axis=0
            )
        return lax.dot_general(
            jnp.ones((SUBLANES, stack.shape[1]), jnp.float32), stack,
            (((1,), (1,)), ((), ())), precision=highest, preferred_element_type=jnp.float32,
        )[:1]

    def inner(a, b):
        return jnp.sum(a * b, axis=0)

    def splat(row, lane):
        return jnp.broadcast_to(row[:, lane:lane + 1], (size_y, size_z))

    def send_all(source, got, send, recv):
        def act(slot, target):
            pltpu.make_async_remote_copy(
                src_ref=source, dst_ref=got.at[slot], send_sem=send, recv_sem=recv,
                device_id=target, device_id_type=MESH,
            ).start()
        for_all(act)

    def take_all(got, send, recv):
        pltpu.make_async_copy(got, got, send).wait()
        pltpu.make_async_copy(got, got, recv).wait()

    lane = iota((size_y, size_z), 1)
    sub = iota((size_y, size_z), 0)

    def column_pack(plane_of, pos):
        pack = jnp.zeros((size_y, size_z), jnp.float32)
        for s in range(solves):
            for x in range(size_x):
                column = jnp.broadcast_to(plane_of(s, x)[:, pos:pos + 1], (size_y, size_z))
                pack = jnp.where(lane == s * size_x + x, column, pack)
        return pack

    def trade(index, source, target):
        def each(act):
            for d, axis in enumerate(AXES):
                if sizes[d] == 1:
                    continue
                for side, step in ((0, -1), (1, 1)):
                    sends = here[d] > 0 if side == 0 else here[d] < sizes[d] - 1
                    takes = here[d] < sizes[d] - 1 if side == 0 else here[d] > 0
                    copy = pltpu.make_async_remote_copy(
                        src_ref=source(d, side), dst_ref=target(d, 1 - side),
                        send_sem=halo_send.at[index, 2 * d + side],
                        recv_sem=halo_recv.at[index, 2 * d + side],
                        device_id={axis: jnp.clip(here[d] + step, 0, sizes[d] - 1)},
                        device_id_type=MESH,
                    )
                    act(copy, sends, takes)

        def start(copy, sends, takes):
            @pl.when(sends)
            def _():
                copy.start()

        def finish(copy, sends, takes):
            @pl.when(takes)
            def _():
                copy.wait_recv()

            @pl.when(sends)
            def _():
                copy.wait_send()

        each(start)
        return lambda: each(finish)

    parts = []
    for load in loads:
        load.wait()
    for s in range(solves):
        for k in range(keep):
            stored = basis[s, k].astype(jnp.float32)
            wide[s, k] = stored
            parts.append(inner(stored, rhs[s]))
    row1[...] = row_of(parts)
    ends_x, ends_y, ends_z = ((0, size - 1) for size in (size_x, size_y, size_z))
    for k in range(keep):
        for side in (0, 1):
            for s in range(solves):
                many_face_y[side, s, k] = jnp.concatenate(
                    [wide[s, k, x, ends_y[side]:ends_y[side] + 1, :] for x in range(size_x)],
                    axis=0,
                )
            many_face_z[side, k] = column_pack(lambda s, x: wide[s, k, x], ends_z[side])
    pl.semaphore_wait(barrier, len(moves))
    send_all(row1, got1, send1, recv1)
    finish_many = trade(
        0,
        lambda d, side: (
            wide.at[:, :, ends_x[side]], many_face_y.at[side], many_face_z.at[side]
        )[d],
        lambda d, side: (many_x, many_y, many_z)[d].at[side],
    )

    row, col = iota((size_z, size_z), 0), iota((size_z, size_z), 1)
    full_z = line_matrix(stiffness[...], row, col)
    area = size_x * size_y
    row, col = iota((area, area), 0), iota((area, area), 1)
    row_x, col_x, row_y, col_y = row // size_y, col // size_y, row % size_y, col % size_y
    full_xy = jnp.where(
        row_y == col_y, line_matrix(stiffness[...], row_x, col_x), 0.0
    ) + jnp.where(row_x == col_x, line_matrix(stiffness[...], row_y, col_y), 0.0)
    for kept, full in ((mat_z, full_z), (mat_xy, full_xy)):
        kept[0], kept[1] = halves(full)
    pairs = [(k, l) for k in range(keep) for l in range(k, keep)]
    gram = [inner(wide[s, k], wide[s, l]) for s in range(solves) for k, l in pairs]
    rows2[1:2] = row_of(gram[:LANES])
    gram_rest = gram[LANES:]

    def exchange(index, field):
        for s in range(solves):
            for side, pos in ((0, 0), (1, size_y - 1)):
                face_y[index, side, s] = jnp.concatenate(
                    [field[s, x, pos:pos + 1, :] for x in range(size_x)], axis=0
                )
        for side, pos in ((0, 0), (1, size_z - 1)):
            face_z[index, side] = column_pack(lambda s, x: field[s, x], pos)
        return trade(
            1 + index,
            lambda d, side: (
                field.at[:, ends_x[side]], face_y.at[index, side], face_z.at[index, side]
            )[d],
            lambda d, side: (ghost_x, ghost_y, ghost_z)[d].at[index, side],
        )

    def local(field, s):
        flat = field[s].reshape(area, size_z)
        high, low = halves(flat)
        dot = functools.partial(jnp.dot, preferred_element_type=jnp.float32)
        along_z = dot(high, mat_z[0]) + (dot(low, mat_z[0]) + dot(high, mat_z[1]))
        along_xy = dot(mat_xy[0], high) + (dot(mat_xy[1], high) + dot(mat_xy[0], low))
        out = (along_z + along_xy).reshape(size_x, size_y, size_z)
        return out + helm[s] * inertia[...] * field[s]

    def coupled(s, ghost_x, ghost_y, ghost_z):
        low_z, high_z = ghost_z(0), ghost_z(1)
        low_y, high_y = ghost_y(0, s), ghost_y(1, s)
        planes = []
        for x in range(size_x):
            spot = s * size_x + x
            plane = jnp.where(lane == 0, jnp.broadcast_to(low_z[:, spot:spot + 1], lane.shape), 0.0)
            plane = jnp.where(
                lane == size_z - 1, jnp.broadcast_to(high_z[:, spot:spot + 1], lane.shape), plane
            )
            plane = plane + jnp.where(
                sub == 0, jnp.broadcast_to(low_y[x:x + 1, :], lane.shape), 0.0
            )
            plane = plane + jnp.where(
                sub == size_y - 1,
                jnp.broadcast_to(high_y[x:x + 1, :], lane.shape), 0.0,
            )
            if x == 0:
                plane = plane + ghost_x(0, s)
            if x == size_x - 1:
                plane = plane + ghost_x(1, s)
            planes.append(plane)
        return penalty * jnp.stack(planes)

    def received(index, s):
        return coupled(
            s,
            lambda side, at: ghost_x[index, side, at],
            lambda side, at: ghost_y[index, side, at],
            lambda side: ghost_z[index, side],
        )

    take_all(got1, send1, recv1)
    coefs = (row1[...] + jnp.sum(got1[...], axis=0)) * inverse
    splats = [[splat(coefs, s * keep + k) for k in range(keep)] for s in range(solves)]
    for s in range(solves):
        total = jnp.zeros((size_x, size_y, size_z), jnp.float32)
        for k in range(keep):
            total = total + splats[s][k][None] * wide[s, k]
        x0[s] = total
    for s in range(solves):
        r0[s] = rhs[s] - local(x0, s)
    by_lane = []
    for k in range(keep):
        mixed = jnp.zeros((size_y, size_z), jnp.float32)
        for s in range(solves):
            mixed = jnp.where(lane // size_x == s, splats[s][k], mixed)
        by_lane.append(mixed)
    finish_many()

    def combined(values):
        return functools.reduce(lambda a, b: a + b, values)

    both_z = [
        combined([by_lane[k] * many_z[side, k] for k in range(keep)]) for side in (0, 1)
    ]
    for s in range(solves):
        r0[s] = r0[s] + coupled(
            s,
            lambda side, at: combined([splats[at][k] * many_x[side, at, k] for k in range(keep)]),
            lambda side, at: combined([splats[at][k] * many_y[side, at, k] for k in range(keep)]),
            lambda side: both_z[side],
        )
    finish = exchange(0, r0)
    for s in range(solves):
        q[s] = local(r0, s)
    with_r = [inner(wide[s, k], r0[s]) for s in range(solves) for k in range(keep)]
    finish()
    for s in range(solves):
        q[s] = q[s] - received(0, s)
    finish = exchange(1, q)
    with_q = [inner(wide[s, k], q[s]) for s in range(solves) for k in range(keep)]
    moments = []
    for s in range(solves):
        moments.append(
            [inner(r0[s], r0[s]), inner(r0[s], q[s]), inner(q[s], q[s]), inner(q[s], local(q, s))]
        )
    flat_moments = [moments[s][j] for s in range(solves) for j in range(4)]
    most = row_of(with_r + with_q + flat_moments + gram_rest)
    finish()
    late = [jnp.zeros((size_y, size_z), jnp.float32)] * (at_m + 4 * solves)
    for s in range(solves):
        late[at_m + 4 * s + 3] = inner(q[s], received(1, s))
    rows2[0:1] = most - row_of(late)
    send_all(rows2, got2, send2, recv2)
    take_all(got2, send2, recv2)
    sums = (rows2[...] + jnp.sum(got2[...], axis=0)) * inverse
    main, other = sums[0:1], sums[1:2]

    for s in range(solves):
        coef = [splat(coefs, s * keep + k) for k in range(keep)]
        by_r = [splat(main, s * keep + k) for k in range(keep)]
        by_q = [splat(main, at_q + s * keep + k) for k in range(keep)]
        m0, m1, m2, m3 = (splat(main, at_m + 4 * s + j) for j in range(4))
        table = {}
        for at, (k, l) in enumerate(pairs):
            spot = s * len(pairs) + at
            value = splat(other, spot) if spot < LANES else splat(main, at_rest + spot - LANES)
            table[k, l] = table[l, k] = value
        first = m0 / m1
        middle = m2 / m1
        across = m3 / m1 - middle * middle
        flat = across <= 1e-6 * middle * middle
        second = jnp.where(flat, 0.0, (1.0 - first * middle) / jnp.where(flat, 1.0, across))
        on_q = second
        on_r = first - second * middle
        moved = [
            functools.reduce(lambda a, b: a + b, [table[k, l] * coef[l] for l in range(keep)])
            for k in range(keep)
        ]
        weight = [moved[k] + on_r * by_r[k] + on_q * by_q[k] for k in range(keep)]
        square = on_r * on_r * m0 + 2.0 * on_r * on_q * m1 + on_q * on_q * m2
        mixed = jnp.zeros_like(square)
        for k in range(keep):
            square = square + coef[k] * (2.0 * weight[k] - moved[k])
            pulled = functools.reduce(
                lambda a, b: a + b, [table[k, l] * weight[l] for l in range(keep)]
            )
            mixed = mixed + weight[k] * (pulled - 2.0 * weight[k])
        scale = lax.rsqrt(square + mixed + epsilon)
        answer = x0[s] + on_r[None] * r0[s] + on_q[None] * q[s]
        sol[s] = answer
        for k in range(keep):
            answer = answer - weight[k][None] * wide[s, k]
        new[s] = answer * scale[None]


def write(sol_in, new_in, sol, new):
    sol[...] = sol_in[...]
    new[...] = new_in[...].astype(jnp.bfloat16)


def on_device(sizes, rhs, basis, inertia, helm, stiffness):
    solves, size_x, size_y, size_z = rhs.shape
    keep = basis.shape[1]
    total_points = float(rhs[0].size * sizes[0] * sizes[1] * sizes[2])
    others = sizes[0] * sizes[1] * sizes[2] - 1
    field = pltpu.VMEM(rhs.shape, jnp.float32)
    vmem = pl.BlockSpec(memory_space=pltpu.VMEM)
    smem = pl.BlockSpec(memory_space=pltpu.SMEM)
    area = size_x * size_y
    faces = (EXCHANGES, 2, solves)
    anywhere = pl.BlockSpec(memory_space=pl.ANY)
    held = pl.pallas_call(
        functools.partial(kernel, sizes, total_points),
        out_shape=(field, field),
        in_specs=[anywhere, anywhere, anywhere, smem, anywhere],
        out_specs=(vmem, vmem),
        scratch_shapes=[
            field,
            pltpu.VMEM(basis.shape, basis.dtype),
            pltpu.VMEM(inertia.shape, inertia.dtype),
            pltpu.VMEM(stiffness.shape, stiffness.dtype),
            pltpu.SemaphoreType.DMA((4,)),
            pltpu.VMEM(basis.shape, jnp.float32),
            field, field, field,
            pltpu.VMEM((2, size_z, size_z), jnp.bfloat16),
            pltpu.VMEM((2, area, area), jnp.bfloat16),
            pltpu.VMEM((*faces, size_x, size_z), jnp.float32),
            pltpu.VMEM((EXCHANGES, 2, size_y, size_z), jnp.float32),
            pltpu.VMEM((*faces, size_y, size_z), jnp.float32),
            pltpu.VMEM((*faces, size_x, size_z), jnp.float32),
            pltpu.VMEM((EXCHANGES, 2, size_y, size_z), jnp.float32),
            pltpu.VMEM((2, solves, keep, size_x, size_z), jnp.float32),
            pltpu.VMEM((2, keep, size_y, size_z), jnp.float32),
            pltpu.VMEM((2, solves, keep, size_y, size_z), jnp.float32),
            pltpu.VMEM((2, solves, keep, size_x, size_z), jnp.float32),
            pltpu.VMEM((2, keep, size_y, size_z), jnp.float32),
            pltpu.VMEM((1, LANES), jnp.float32),
            pltpu.VMEM((2, LANES), jnp.float32),
            pltpu.VMEM((others, 1, LANES), jnp.float32),
            pltpu.VMEM((others, 2, LANES), jnp.float32),
            pltpu.SemaphoreType.DMA((1 + EXCHANGES, 6)),
            pltpu.SemaphoreType.DMA((1 + EXCHANGES, 6)),
            pltpu.SemaphoreType.DMA,
            pltpu.SemaphoreType.DMA,
            pltpu.SemaphoreType.DMA,
            pltpu.SemaphoreType.DMA,
        ],
        compiler_params=pltpu.CompilerParams(collective_id=0, has_side_effects=True),
    )(rhs, basis, inertia, helm, stiffness)
    return pl.pallas_call(
        write,
        out_shape=(
            jax.ShapeDtypeStruct(rhs.shape, jnp.float32),
            jax.ShapeDtypeStruct(rhs.shape, jnp.bfloat16),
        ),
        in_specs=[vmem, vmem],
        out_specs=(vmem, vmem),
    )(*(pltpu.with_memory_space_constraint(part, pltpu.VMEM) for part in held))


def solution(mesh):
    placed = (
        P(None, "gx", "gy", "gz"),
        P(None, None, "gx", "gy", "gz"),
        P("gx", "gy", "gz"),
        P(),
        P(),
    )
    sizes = tuple(mesh.shape[axis] for axis in AXES)
    return jax.shard_map(
        functools.partial(on_device, sizes),
        mesh=mesh,
        in_specs=placed,
        out_specs=(P(None, "gx", "gy", "gz"), P(None, "gx", "gy", "gz")),
        check_vma=False,
    )
```
